32 devices in a mesh: grp: 2 (over x), layer: 4 (over z), feat: 4 (over y, core).
Axes of the slice: x: 2, y: 2, z: 4, core: 2. Of those that a mesh axis runs over, the one named last changes fastest.
Arguments:
- inputs: bfloat16 [4, 512, 2304], P('layer', ('grp', 'feat')), may hold values from -6 to 6
- targets: bfloat16 [512, 4, 2304], P(('grp', 'feat'), None, 'layer'), may hold values from -6 to 6
- enc_weight: bfloat16 [4, 2304, 8192], P('layer', None, 'feat'), may hold values from -0.125 to 0.125
- enc_bias: float32 [4, 8192], P('layer', 'feat'), may hold values from -3 to 3
- dec_weight: bfloat16 [10, 8192, 2304], P(None, 'feat', 'layer'), may hold values from -0.0625 to 0.0625
- dec_bias: float32 [4, 2304], P(None, 'layer'), may hold values from -3 to 3
Outputs:
- enc_grad: bfloat16 [4, 2304, 8192], P('layer', 'grp', 'feat')
- enc_bias_grad: float32 [4, 8192], P('layer', 'feat')
- dec_grad: bfloat16 [10, 8192, 2304], P('grp', 'feat', 'layer')
- dec_bias_grad: float32 [4, 2304], P(None, 'layer')
The draws below stay inside these ranges and needn't reach their ends.
All inputs are finite; a program needn't handle non-finite values.
Results may differ from the reference program's by a relative error of at most 0.019.
Values may be sent and summed in bfloat16 or wider, within the bound.
A program may use at most 128 MiB of HBM per device.

```python
import jax
import jax.numpy as jnp

D = 2304
FEATS = 8192
LAYERS = 4
PAIRS = 10
TOKENS = 512


def block_scale(own_key, shape, pieces, least, top_value):
    level = 1.0
    for axis_at, parts in pieces:
        steps = jax.random.uniform(jax.random.fold_in(jax.random.fold_in(own_key, 6), axis_at), (parts,), jnp.float32, least / len(pieces), top_value / len(pieces))
        level = level * jnp.repeat(jnp.exp(steps), shape[axis_at] // parts).reshape((-1,) + (1,) * (len(shape) - 1 - axis_at))
    return level


def gaussian(rng, dims, deviation, bound, cuts=(), held_as=jnp.bfloat16):
    values = jax.random.normal(rng, dims, jnp.float32) * deviation
    if len(cuts) > 0:
        values = block_scale(rng, dims, cuts, -0.22, 0.18) * values
    return jnp.clip(values, min=-bound, max=bound).astype(held_as)


def setup_inputs(seed: int = 0) -> dict:
    streams_of = jax.random.split(jax.random.key(seed), 7)
    inputs = gaussian(streams_of[0], (LAYERS, TOKENS, D), 1.0, 6.0, ((0, 4), (1, 8)))
    targets = gaussian(streams_of[1], (TOKENS, LAYERS, D), 1.0, 6.0, ((0, 8), (2, 4)))
    enc_weight = gaussian(streams_of[2], (LAYERS, D, FEATS), D ** -0.5, 0.125, ((0, 4), (2, 4)))
    enc_bias = gaussian(streams_of[3], (LAYERS, FEATS), 0.5, 3.0, ((0, 4), (1, 4)), jnp.float32)
    dec_weight = gaussian(streams_of[4], (PAIRS, FEATS, D), FEATS ** -0.5, 0.0625, ((1, 4), (2, 4)))
    dec_bias = gaussian(streams_of[5], (LAYERS, D), 0.5, 3.0, ((1, 4),), jnp.float32)
    return dict(inputs=inputs, targets=targets, enc_weight=enc_weight, enc_bias=enc_bias, dec_weight=dec_weight, dec_bias=dec_bias)


def pair_list(count):
    return [(source, target) for source in range(count) for target in range(source, count)]


def reference(inputs, targets, enc_weight, enc_bias, dec_weight, dec_bias):
    pairs = pair_list(LAYERS)
    pre = [jnp.dot(inputs[s], enc_weight[s], preferred_element_type=jnp.float32) + enc_bias[s] for s in range(LAYERS)]
    acts = [jnp.maximum(value, 0.0).astype(jnp.bfloat16) for value in pre]
    errors = []
    for target in range(LAYERS):
        total = jnp.zeros((TOKENS, D), jnp.float32) + dec_bias[target].astype(jnp.float32)
        for index, (source, later) in enumerate(pairs):
            if later == target:
                total = total + jnp.dot(acts[source], dec_weight[index], preferred_element_type=jnp.float32)
        errors.append(total - targets[:, target, :].astype(jnp.float32))
    dec_bias_grad = jnp.stack([jnp.sum(value, axis=0) for value in errors]) / TOKENS
    derr = [(value / TOKENS).astype(jnp.bfloat16) for value in errors]
    dec_grad = jnp.stack([jnp.dot(acts[s].T, derr[t], preferred_element_type=jnp.float32) for (s, t) in pairs]).astype(jnp.bfloat16)
    enc_grads = []
    bias_grads = []
    for source in range(LAYERS):
        dacts = jnp.zeros((TOKENS, FEATS), jnp.float32)
        for index, (first, target) in enumerate(pairs):
            if first == source:
                dacts = dacts + jnp.dot(derr[target], dec_weight[index].T, preferred_element_type=jnp.float32)
        dpre = jnp.where(pre[source] > 0, dacts, jnp.zeros_like(dacts))
        bias_grads.append(jnp.sum(dpre, axis=0))
        enc_grads.append(jnp.dot(inputs[source].T, dpre.astype(jnp.bfloat16), preferred_element_type=jnp.float32).astype(jnp.bfloat16))
    return jnp.stack(enc_grads), jnp.stack(bias_grads), dec_grad, dec_bias_grad
```

```python
import jax
import jax.numpy as jnp
from jax import lax
from jax.sharding import PartitionSpec as P


def pair_list(count):
    return [(source, target) for source in range(count) for target in range(source, count)]


def per_device(inputs, targets, enc_weight, enc_bias, dec_weight, dec_bias):
    layers = lax.axis_size("layer")
    feat_count = lax.axis_size("feat")
    group_count = lax.axis_size("grp")
    pairs = pair_list(layers)
    tok_dev, width = inputs.shape[1], inputs.shape[2]
    group_tokens = tok_dev * feat_count
    total_tokens = group_tokens * group_count
    block = dec_weight.shape[2]
    feats = dec_weight.shape[1]
    rows = lax.all_gather(inputs[0], "feat", axis=0, tiled=True)
    pre = jnp.dot(rows, enc_weight[0], preferred_element_type=jnp.float32) + enc_bias[0]
    acts = jnp.maximum(pre, 0.0).astype(jnp.bfloat16)
    sources = lax.all_gather(acts, "layer", axis=0, tiled=False)

    group = lax.axis_index("grp")
    own_width = width // group_count
    shifts = range(1, group_count)

    def shifted(value, shift):
        return lax.ppermute(
            value, "grp", [(g, (g + shift) % group_count) for g in range(group_count)]
        )

    def with_others(value, axis):
        return jnp.concatenate([value] + [shifted(value, k) for k in shifts], axis=axis)

    def column_block(shift):
        owner = lax.rem(group + shift, group_count)
        return lax.dynamic_slice_in_dim(rows, owner * own_width, own_width, axis=1)

    all_columns = jnp.concatenate(
        [column_block(0)] + [shifted(column_block(k), k) for k in shifts], axis=0
    )
    all_sources = with_others(sources, 1)

    def decode_target(target):
        total = jnp.zeros((group_tokens, block), jnp.float32)
        for index, (source, later) in enumerate(pairs):
            if later == target:
                total = total + jnp.dot(
                    sources[source], dec_weight[index], preferred_element_type=jnp.float32
                )
        return total.astype(jnp.bfloat16).reshape(feat_count, tok_dev, block)

    partial = jnp.stack([decode_target(target) for target in range(layers)], axis=1)
    recon = lax.psum_scatter(
        partial.reshape(feat_count * layers * tok_dev, block),
        "feat",
        scatter_dimension=0,
        tiled=True,
    )
    recon = recon.reshape(layers, tok_dev, block).astype(jnp.float32)
    wanted = jnp.swapaxes(targets, 0, 1).astype(jnp.float32)
    errors = recon + dec_bias[:, None, :] - wanted
    dec_bias_grad = lax.psum(jnp.sum(errors, axis=1), ("grp", "feat")) / total_tokens
    derr_own = (errors / total_tokens).astype(jnp.bfloat16)
    gathered = lax.all_gather(
        derr_own.reshape(layers * tok_dev, block), "feat", axis=0, tiled=True
    )
    gathered = gathered.reshape(feat_count, layers, tok_dev, block)
    derr = jnp.stack(
        [gathered[:, target].reshape(group_tokens, block) for target in range(layers)]
    )
    all_errors = with_others(derr, 1)
    per_group = len(pairs) // group_count

    partials = []
    for source in range(layers):
        total = jnp.zeros((group_tokens, feats), jnp.float32)
        for index, (first, target) in enumerate(pairs):
            if first == source:
                total = total + jnp.einsum(
                    "rd,fd->rf",
                    derr[target],
                    dec_weight[index],
                    preferred_element_type=jnp.float32,
                )
        partials.append(total.astype(jnp.bfloat16))
    dacts = lax.psum_scatter(
        jnp.concatenate(partials, axis=0), "layer", scatter_dimension=0, tiled=True
    ).astype(jnp.float32)
    dpre = jnp.where(pre > 0, dacts, jnp.zeros_like(dacts))
    enc_bias_grad = lax.psum(jnp.sum(dpre, axis=0), "grp")[None]
    all_dpre = with_others(dpre.astype(jnp.bfloat16), 0)

    starts = [group * per_group for group in range(group_count)]
    chosen_s = jnp.array([[s for s, _ in pairs[a : a + per_group]] for a in starts])
    chosen_t = jnp.array([[t for _, t in pairs[a : a + per_group]] for a in starts])

    def pair_grad(slot):
        left = lax.dynamic_index_in_dim(all_sources, chosen_s[group, slot], 0, False)
        right = lax.dynamic_index_in_dim(all_errors, chosen_t[group, slot], 0, False)
        return jnp.einsum("rf,rd->fd", left, right, preferred_element_type=jnp.float32).astype(
            jnp.bfloat16
        )

    dec_grad = jnp.stack([pair_grad(slot) for slot in range(per_group)])
    enc_grad = jnp.einsum(
        "rd,rf->df", all_columns, all_dpre, preferred_element_type=jnp.float32
    ).astype(jnp.bfloat16)[None]
    return (enc_grad, enc_bias_grad, dec_grad, dec_bias_grad)


def solution(mesh):
    return jax.shard_map(
        per_device,
        mesh=mesh,
        in_specs=(
            P("layer", ("grp", "feat"), None),
            P(("grp", "feat"), None, "layer"),
            P("layer", None, "feat"),
            P("layer", "feat"),
            P(None, "feat", "layer"),
            P(None, "layer"),
        ),
        out_specs=(
            P("layer", "grp", "feat"),
            P("layer", "feat"),
            P("grp", "feat", "layer"),
            P(None, "layer"),
        ),
        check_vma=False,
    )
```
